32 devices in a mesh: rows: 4 (over z), cols: 2 (over x), slabs: 4 (over y, core).
Axes of the slice: x: 2, y: 2, z: 4, core: 2. Of those that a mesh axis runs over, the one named last changes fastest.
Arguments:
- pressure: float32 [512, 8, 128, 128], P('rows', 'cols', 'slabs'), may hold values from 0.5 to 2
- earlier: float32 [512, 8, 128, 128], P('rows', 'cols', 'slabs'), may hold values from 0.2 to 1.8
- speed_square: float32 [512, 8, 128, 128], P('rows', 'cols', 'slabs'), may hold values from 0.05 to 0.3
Outputs:
- scaled_field: float32 [512, 8, 128, 128], P('rows', 'cols', 'slabs')
- pressure_end: float32 [512, 8, 128, 128], P('rows', 'cols', 'slabs')
The draws below stay inside these ranges and needn't reach their ends.
All inputs are finite; a program needn't handle non-finite values.
Results may differ from the reference program's by a relative error of at most 0.00002.
Values sent between devices are 32-bit elements; how exact they have to be, the bound alone decides.
A program may use at most 128 MiB of HBM per device.

```python
import jax
import jax.numpy as jnp
from jax import lax

GRID_J = 512
GRID_I = 8
GRID_K = 128
MEMBERS = 128
STEPS = 3


def block_scale(key, extent, pieces, least, top_value):
    loudness, own = 1.0, jax.random.fold_in(key, 6)
    for position, blocks in pieces:
        heights = jnp.exp(jax.random.uniform(jax.random.fold_in(own, position), (blocks,), jnp.float32, least / len(pieces), top_value / len(pieces)))
        loudness = loudness * jnp.repeat(heights, extent[position] // blocks).reshape([-1 if axis == position else 1 for axis in range(len(extent))])
    return loudness


def setup_inputs(seed: int = 0) -> dict:
    streams_of = jax.random.split(jax.random.key(seed), 4)
    pressure = jnp.clip(0.5 + 1.5 * jax.random.uniform(streams_of[0], (GRID_J, GRID_I, GRID_K, MEMBERS), jnp.float32) ** block_scale(streams_of[0], (GRID_J, GRID_I, GRID_K, MEMBERS), ((0, 4), (1, 2), (2, 4)), -0.2, 0.2), 0.5, 2.0)
    earlier = jnp.clip(0.2 + 1.5999999 * jax.random.uniform(streams_of[1], (GRID_J, GRID_I, GRID_K, MEMBERS), jnp.float32) ** block_scale(streams_of[1], (GRID_J, GRID_I, GRID_K, MEMBERS), ((0, 4), (1, 2), (2, 4)), -0.2, 0.2), 0.2, 1.8)
    speed_square = jnp.clip(0.05 + 0.25 * jax.random.uniform(streams_of[2], (GRID_J, GRID_I, GRID_K, MEMBERS), jnp.float32) ** block_scale(streams_of[2], (GRID_J, GRID_I, GRID_K, MEMBERS), ((0, 4), (1, 2), (2, 4)), -0.2, 0.2), 0.05, 0.3)
    return dict(pressure=pressure, earlier=earlier, speed_square=speed_square)


def strip_edges(values, dims):
    for dim in dims:
        values = lax.slice_in_dim(values, 1, values.shape[dim] - 1, axis=dim)
    return values

def neighbour(values, dim, start, dims):
    others = [other for other in dims if other != dim]
    values = strip_edges(values, others)
    return lax.slice_in_dim(values, start, start + values.shape[dim] - 2, axis=dim)

def one_step(padded, before, speed_square):
    middle = strip_edges(padded, (0, 1, 2))
    lower = [neighbour(padded, dim, 0, (0, 1, 2)) for dim in (0, 1, 2)]
    upper = [neighbour(padded, dim, 2, (0, 1, 2)) for dim in (0, 1, 2)]
    spread = lower[0] + upper[0] + lower[1] + upper[1] + lower[2] + upper[2] - 6.0 * middle
    return 2.0 * middle - before + speed_square * spread

def reference(pressure, earlier, speed_square):
    for step in range(STEPS):
        later = one_step(jnp.pad(pressure, ((1, 1), (1, 1), (1, 1), (0, 0)), mode='wrap'), earlier, speed_square)
        earlier, pressure = (pressure, later)
    line_mean = lax.optimization_barrier(jnp.mean(pressure, axis=0, keepdims=True))
    centred = pressure - line_mean
    line_variance = lax.optimization_barrier(jnp.mean(centred * centred, axis=0, keepdims=True))
    scaled_field = centred * lax.rsqrt(line_variance + 0.0001)
    return (scaled_field, pressure)
```

```python
import functools

import jax
import jax.numpy as jnp
from jax import lax
from jax.experimental import pallas as pl
from jax.experimental.pallas import tpu as pltpu
from jax.sharding import PartitionSpec as P

STEPS = 3
GUESS = 1.0
EPS = 0.0001
MESH = pl.DeviceIdType.MESH
TILE = 8
LO, HI = 0, 1


def leapfrog(sizes, p_hbm, e_hbm, s_hbm, out_hbm, stat_hbm,
             even, odd, speed, xh, yh, line, stat,
             xs, xr, ys, yr, zs, zr, ls, lr, own, out_sem):
    rows, cols, slabs = sizes
    planes, cells, depth = p_hbm.shape[0], p_hbm.shape[1], p_hbm.shape[2]
    tiles = depth // TILE
    body_planes = pl.ds(1, planes)
    row, col, slab = (lax.axis_index(name) for name in ("rows", "cols", "slabs"))

    def shifted(name, index, count, by):
        return {name: lax.rem(index + by + count, count)}

    x_to = (shifted("cols", col, cols, -1), shifted("cols", col, cols, 1))
    y_to = (shifted("slabs", slab, slabs, -1), shifted("slabs", slab, slabs, 1))
    z_to = (shifted("rows", row, rows, -1), shifted("rows", row, rows, 1))
    peers = [shifted("rows", row, rows, d) for d in range(1, rows)]

    loads = [
        pltpu.make_async_copy(p_hbm, even.at[body_planes], own.at[0]),
        pltpu.make_async_copy(e_hbm, odd.at[body_planes], own.at[1]),
        pltpu.make_async_copy(s_hbm, speed, own.at[2]),
    ]
    for load in loads:
        load.start()

    barrier = pltpu.get_barrier_semaphore()
    greeted = list(x_to) + list(y_to) + peers
    for device in greeted:
        pl.semaphore_signal(barrier, inc=1, device_id=device, device_id_type=MESH)
    pl.semaphore_wait(barrier, len(greeted))

    fields = (even, odd)

    def remote(src, dst, send, recv, device):
        return pltpu.make_async_remote_copy(
            src_ref=src, dst_ref=dst, send_sem=send, recv_sem=recv,
            device_id=device, device_id_type=MESH,
        )

    def source(step):
        return p_hbm if step == 0 else fields[step % 2].at[body_planes]

    def x_copy(step, side, q):
        cell = 0 if side == LO else cells - 1
        part = pl.ds(q * TILE, TILE)
        return remote(source(step).at[:, cell, part, :], xh.at[step, 1 - side, :, part, :],
                      xs.at[step, side, q], xr.at[step, side, q], x_to[side])

    def y_copy(step, side):
        part = pl.ds(0 if side == LO else depth - TILE, TILE)
        return remote(source(step).at[:, :, part, :], yh.at[step, 1 - side],
                      ys.at[step, side], yr.at[step, side], y_to[side])

    def z_copy(step, side):
        src = p_hbm.at[0 if side == LO else planes - 1] if step == 0 else (
            fields[step % 2].at[1 if side == LO else planes])
        dst = fields[step % 2].at[planes + 1 if side == LO else 0]
        return remote(src, dst, zs.at[step, side], zr.at[step, side], z_to[side])

    def order(step):
        return (LO, HI) if step % 2 == 0 else (HI, LO)

    def update(step, cell, q, low, high):
        now, then = fields[step % 2], fields[(step + 1) % 2]
        part = pl.ds(q * TILE, TILE)
        index = lax.broadcasted_iota(jnp.int32, (TILE, TILE, 128), 1)
        last = step == STEPS - 1

        def block(b, sums):
            j = b * TILE
            here, padded = pl.ds(j, TILE), pl.ds(j + 1, TILE)
            mid = now[padded, cell, part, :]
            if q == 0:
                below = yh[step, LO, here, cell, TILE - 1:TILE, :]
            else:
                below = now[padded, cell, q * TILE - 1:q * TILE, :]
            if q == tiles - 1:
                above = yh[step, HI, here, cell, 0:1, :]
            else:
                above = now[padded, cell, (q + 1) * TILE:(q + 1) * TILE + 1, :]
            k_low = jnp.where(index == 0, below, pltpu.roll(mid, 1, 1))
            k_high = jnp.where(index == TILE - 1, above, pltpu.roll(mid, TILE - 1, 1))
            spread = (now[here, cell, part, :] + now[pl.ds(j + 2, TILE), cell, part, :]
                      + low(here, padded, part) + high(here, padded, part)
                      + k_low + k_high - 6.0 * mid)
            new = 2.0 * mid - then[padded, cell, part, :] + speed[here, cell, part, :] * spread
            then[padded, cell, part, :] = new
            if last:
                moved = new - GUESS
                return sums[0] + jnp.sum(moved, axis=0), sums[1] + jnp.sum(moved * moved, axis=0)
            return sums

        zero = jnp.zeros((TILE, 128), jnp.float32)
        sums = lax.fori_loop(0, planes // TILE, block, (zero, zero) if last else 0)
        if last:
            line[row, cell, 0, part, :] = sums[0]
            line[row, cell, 1, part, :] = sums[1]

    def edge(step, side, q):
        now = fields[step % 2]
        halo = lambda here, padded, part: xh[step, side, here, part, :]
        if side == LO:
            update(step, 0, q, halo, lambda here, padded, part: now[padded, 1, part, :])
        else:
            update(step, cells - 1, q, lambda here, padded, part: now[padded, cells - 2, part, :], halo)

    def interior(step):
        now = fields[step % 2]

        def at(cell, carry):
            for q in range(tiles):
                update(step, cell, q,
                       lambda here, padded, part: now[padded, cell - 1, part, :],
                       lambda here, padded, part: now[padded, cell + 1, part, :])
            return carry

        lax.fori_loop(1, cells - 1, at, 0)

    def line_copies(cell):
        return [remote(line.at[row, cell], line.at[row, cell], ls.at[cell, d], lr.at[cell, d], device)
                for d, device in enumerate(peers)]

    def out_copy(cell):
        return pltpu.make_async_copy(odd.at[body_planes, cell], out_hbm.at[:, cell], out_sem.at[cell])

    def finished(cell):
        out_copy(cell).start()
        for copy in line_copies(cell):
            copy.start()

    for side in order(0):
        for q in range(tiles):
            x_copy(0, side, q).start()
    for side in (LO, HI):
        z_copy(0, side).start()
        y_copy(0, side).start()
    for load in loads:
        load.wait()

    for step in range(STEPS):
        if step >= 1:
            for side in order(step - 1):
                z_copy(step - 1, side).wait_send()
                y_copy(step - 1, side).wait_send()
                for q in range(tiles):
                    x_copy(step - 1, side, q).wait_send()
        for side in (LO, HI):
            z_copy(step, side).wait_recv()
            y_copy(step, side).wait_recv()
        interior(step)
        if step == STEPS - 1:
            for cell in range(1, cells - 1):
                finished(cell)
        for side in order(step):
            for q in range(tiles):
                x_copy(step, side, q).wait_recv()
                edge(step, 1 - side, q)
                if step < STEPS - 1:
                    x_copy(step + 1, 1 - side, q).start()
            if step == STEPS - 1:
                finished(0 if side == HI else cells - 1)
        if step < STEPS - 1:
            for side in (LO, HI):
                z_copy(step + 1, side).start()
                y_copy(step + 1, side).start()

    for side in order(STEPS - 1):
        z_copy(STEPS - 1, side).wait_send()
        y_copy(STEPS - 1, side).wait_send()
        for q in range(tiles):
            x_copy(STEPS - 1, side, q).wait_send()

    count = float(planes * rows)
    for cell in range(cells):
        for copy in line_copies(cell):
            copy.wait()
        total, square = line[0, cell, 0], line[0, cell, 1]
        for r in range(1, rows):
            total, square = total + line[r, cell, 0], square + line[r, cell, 1]
        shift = total / count
        stat[0, cell] = GUESS + shift
        stat[1, cell] = lax.rsqrt(square / count - shift * shift + EPS)
    stat_copy = pltpu.make_async_copy(stat, stat_hbm, own.at[0])
    stat_copy.start()
    for cell in range(cells):
        out_copy(cell).wait()
    stat_copy.wait()


def rescale(p_ref, stat_ref, scaled_ref, end_ref):
    mean, scale = stat_ref[0], stat_ref[1]

    def plane(j, carry):
        value = p_ref[j]
        end_ref[j] = value
        scaled_ref[j] = (value - mean) * scale
        return carry

    lax.fori_loop(0, p_ref.shape[0], plane, 0)


def shards(sizes, pressure, earlier, speed_square):
    rows = sizes[0]
    planes, cells, depth, members = pressure.shape
    tiles = depth // TILE
    any_space = pl.BlockSpec(memory_space=pl.ANY)
    dma = pltpu.SemaphoreType.DMA
    end, stat = pl.pallas_call(
        functools.partial(leapfrog, sizes),
        out_shape=(
            jax.ShapeDtypeStruct(pressure.shape, jnp.float32),
            jax.ShapeDtypeStruct((2, cells, depth, members), jnp.float32),
        ),
        in_specs=[any_space] * 3,
        out_specs=(any_space, any_space),
        scratch_shapes=[
            pltpu.VMEM((planes + 2, cells, depth, members), jnp.float32),
            pltpu.VMEM((planes + 2, cells, depth, members), jnp.float32),
            pltpu.VMEM((planes, cells, depth, members), jnp.float32),
            pltpu.VMEM((STEPS, 2, planes, depth, members), jnp.float32),
            pltpu.VMEM((STEPS, 2, planes, cells, TILE, members), jnp.float32),
            pltpu.VMEM((rows, cells, 2, depth, members), jnp.float32),
            pltpu.VMEM((2, cells, depth, members), jnp.float32),
            dma((STEPS, 2, tiles)), dma((STEPS, 2, tiles)),
            dma((STEPS, 2)), dma((STEPS, 2)),
            dma((STEPS, 2)), dma((STEPS, 2)),
            dma((cells, rows - 1)), dma((cells, rows - 1)),
            dma((3,)), dma((cells,)),
        ],
        compiler_params=pltpu.CompilerParams(
            collective_id=0, has_side_effects=True, vmem_limit_bytes=60 * 1024 * 1024
        ),
    )(pressure, earlier, speed_square)

    block = (TILE, cells, depth, members)
    spec = pl.BlockSpec(block, lambda j: (j, 0, 0, 0))
    return pl.pallas_call(
        rescale,
        grid=(planes // TILE,),
        out_shape=(jax.ShapeDtypeStruct(pressure.shape, jnp.float32),) * 2,
        in_specs=[spec, pl.BlockSpec((2, cells, depth, members), lambda j: (0, 0, 0, 0))],
        out_specs=(spec, spec),
    )(end, stat)


def solution(mesh):
    spec = P("rows", "cols", "slabs", None)
    sizes = tuple(mesh.shape[name] for name in ("rows", "cols", "slabs"))
    return jax.shard_map(functools.partial(shards, sizes), mesh=mesh,
                         in_specs=(spec,) * 3, out_specs=(spec,) * 2, check_vma=False)
```

```python
import functools

import jax
import jax.numpy as jnp
from jax import lax
from jax.experimental import pallas as pl
from jax.experimental.pallas import tpu as pltpu
from jax.sharding import PartitionSpec as P

STEPS = 3
GUESS = 1.0
EPS = 0.0001
MESH = pl.DeviceIdType.MESH
TILE = 8
LO, HI = 0, 1


def leapfrog(sizes, p_hbm, e_hbm, s_hbm, end, stat,
             even, odd, xh, yh, line,
             xs, xr, ys, yr, zs, zr, ls, lr, own):
    speed = end
    rows, cols, slabs = sizes
    planes, cells, depth = p_hbm.shape[0], p_hbm.shape[1], p_hbm.shape[2]
    tiles = depth // TILE
    body_planes = pl.ds(1, planes)
    row, col, slab = (lax.axis_index(name) for name in ("rows", "cols", "slabs"))

    def shifted(name, index, count, by):
        return {name: lax.rem(index + by + count, count)}

    x_to = (shifted("cols", col, cols, -1), shifted("cols", col, cols, 1))
    y_to = (shifted("slabs", slab, slabs, -1), shifted("slabs", slab, slabs, 1))
    z_to = (shifted("rows", row, rows, -1), shifted("rows", row, rows, 1))
    peers = [shifted("rows", row, rows, d) for d in range(1, rows)]

    loads = [
        pltpu.make_async_copy(p_hbm, even.at[body_planes], own.at[0]),
        pltpu.make_async_copy(e_hbm, odd.at[body_planes], own.at[1]),
        pltpu.make_async_copy(s_hbm, speed, own.at[2]),
    ]
    for load in loads:
        load.start()

    barrier = pltpu.get_barrier_semaphore()
    greeted = list(x_to) + list(y_to) + peers
    for device in greeted:
        pl.semaphore_signal(barrier, inc=1, device_id=device, device_id_type=MESH)
    pl.semaphore_wait(barrier, len(greeted))

    fields = (even, odd)
    count = float(planes * rows)

    def line_copies(cell, q):
        part = line.at[row, cell, q]
        return [remote(part, part, ls.at[cell, q, d], lr.at[cell, q, d], device)
                for d, device in enumerate(peers)]

    def remote(src, dst, send, recv, device):
        return pltpu.make_async_remote_copy(
            src_ref=src, dst_ref=dst, send_sem=send, recv_sem=recv,
            device_id=device, device_id_type=MESH,
        )

    def source(step):
        return p_hbm if step == 0 else fields[step % 2].at[body_planes]

    def x_copy(step, side, q):
        cell = 0 if side == LO else cells - 1
        part = pl.ds(q * TILE, TILE)
        return remote(source(step).at[:, cell, part, :], xh.at[step, 1 - side, :, part, :],
                      xs.at[step, side, q], xr.at[step, side, q], x_to[side])

    def y_copy(step, side):
        part = pl.ds(0 if side == LO else depth - TILE, TILE)
        return remote(source(step).at[:, :, part, :], yh.at[step, 1 - side],
                      ys.at[step, side], yr.at[step, side], y_to[side])

    def z_copy(step, side):
        src = p_hbm.at[0 if side == LO else planes - 1] if step == 0 else (
            fields[step % 2].at[1 if side == LO else planes])
        dst = fields[step % 2].at[planes + 1 if side == LO else 0]
        return remote(src, dst, zs.at[step, side], zr.at[step, side], z_to[side])

    def order(step):
        return (LO, HI) if step % 2 == 0 else (HI, LO)

    def update(step, cell, q, low, high):
        now, then = fields[step % 2], fields[(step + 1) % 2]
        part = pl.ds(q * TILE, TILE)
        index = lax.broadcasted_iota(jnp.int32, (TILE, TILE, 128), 1)
        last = step == STEPS - 1

        def block(b, sums):
            j = b * TILE
            here, padded = pl.ds(j, TILE), pl.ds(j + 1, TILE)
            mid = now[padded, cell, part, :]
            if q == 0:
                below = yh[step, LO, here, cell, TILE - 1:TILE, :]
            else:
                below = now[padded, cell, q * TILE - 1:q * TILE, :]
            if q == tiles - 1:
                above = yh[step, HI, here, cell, 0:1, :]
            else:
                above = now[padded, cell, (q + 1) * TILE:(q + 1) * TILE + 1, :]
            k_low = jnp.where(index == 0, below, pltpu.roll(mid, 1, 1))
            k_high = jnp.where(index == TILE - 1, above, pltpu.roll(mid, TILE - 1, 1))
            spread = (now[here, cell, part, :] + now[pl.ds(j + 2, TILE), cell, part, :]
                      + low(here, padded, part) + high(here, padded, part)
                      + k_low + k_high - 6.0 * mid)
            new = 2.0 * mid - then[padded, cell, part, :] + speed[here, cell, part, :] * spread
            if last:
                end[here, cell, part, :] = new
                moved = new - GUESS
                return sums[0] + jnp.sum(moved, axis=0), sums[1] + jnp.sum(moved * moved, axis=0)
            then[padded, cell, part, :] = new
            return sums

        zero = jnp.zeros((TILE, 128), jnp.float32)
        sums = lax.fori_loop(0, planes // TILE, block, (zero, zero) if last else 0)
        if last:
            line[row, cell, q, 0] = sums[0]
            line[row, cell, q, 1] = sums[1]
            for copy in line_copies(cell, q):
                copy.start()

    def edge(step, side, q):
        now = fields[step % 2]
        halo = lambda here, padded, part: xh[step, side, here, part, :]
        if side == LO:
            update(step, 0, q, halo, lambda here, padded, part: now[padded, 1, part, :])
        else:
            update(step, cells - 1, q, lambda here, padded, part: now[padded, cells - 2, part, :], halo)

    def interior(step):
        now = fields[step % 2]

        def at(cell, carry):
            for q in range(tiles):
                update(step, cell, q,
                       lambda here, padded, part: now[padded, cell - 1, part, :],
                       lambda here, padded, part: now[padded, cell + 1, part, :])
            return carry

        lax.fori_loop(1, cells - 1, at, 0)

    def settle(cell):
        for q in range(tiles):
            for copy in line_copies(cell, q):
                copy.wait()
            total, square = line[0, cell, q, 0], line[0, cell, q, 1]
            for r in range(1, rows):
                total, square = total + line[r, cell, q, 0], square + line[r, cell, q, 1]
            shift = total / count
            part = pl.ds(q * TILE, TILE)
            stat[0, cell, part, :] = GUESS + shift
            stat[1, cell, part, :] = lax.rsqrt(square / count - shift * shift + EPS)

    for side in order(0):
        for q in range(tiles):
            x_copy(0, side, q).start()
    for side in (LO, HI):
        z_copy(0, side).start()
        y_copy(0, side).start()
    for load in loads:
        load.wait()

    for step in range(STEPS):
        if step >= 1:
            for side in order(step - 1):
                z_copy(step - 1, side).wait_send()
                y_copy(step - 1, side).wait_send()
                for q in range(tiles):
                    x_copy(step - 1, side, q).wait_send()
        for side in (LO, HI):
            z_copy(step, side).wait_recv()
            y_copy(step, side).wait_recv()
        interior(step)
        for side in order(step):
            for q in range(tiles):
                x_copy(step, side, q).wait_recv()
                edge(step, 1 - side, q)
                if step < STEPS - 1:
                    x_copy(step + 1, 1 - side, q).start()
            if step == STEPS - 1 and side == order(step)[0]:
                for cell in range(1, cells - 1):
                    settle(cell)
        if step < STEPS - 1:
            for side in (LO, HI):
                z_copy(step + 1, side).start()
                y_copy(step + 1, side).start()

    for side in order(STEPS - 1):
        z_copy(STEPS - 1, side).wait_send()
        y_copy(STEPS - 1, side).wait_send()
        for q in range(tiles):
            x_copy(STEPS - 1, side, q).wait_send()

    for side in order(STEPS - 1):
        settle(0 if side == HI else cells - 1)


def rescale(p_ref, stat_ref, scaled_hbm, end_hbm, scaled, end_sem, scaled_sem):
    planes, parts = p_ref.shape[0], end_sem.shape[0]
    each = planes // parts
    copies = []
    for c in range(parts):
        part = pl.ds(c * each, each)
        copies.append((pltpu.make_async_copy(p_ref.at[part], end_hbm.at[part], end_sem.at[c]),
                       pltpu.make_async_copy(scaled.at[part], scaled_hbm.at[part], scaled_sem.at[c])))

    for c in range(parts):
        copies[c][0].start()

        def plane(j, carry):
            scaled[j] = (p_ref[j] - stat_ref[0]) * stat_ref[1]
            return carry

        lax.fori_loop(c * each, (c + 1) * each, plane, 0, unroll=2)
        copies[c][1].start()
    for pair in copies:
        for copy in pair:
            copy.wait()


def shards(sizes, pressure, earlier, speed_square):
    rows = sizes[0]
    planes, cells, depth, members = pressure.shape
    tiles = depth // TILE
    any_space = pl.BlockSpec(memory_space=pl.ANY)
    dma = pltpu.SemaphoreType.DMA
    vmem_space = pl.BlockSpec(memory_space=pltpu.VMEM)
    end, stat = pl.pallas_call(
        functools.partial(leapfrog, sizes),
        out_shape=(
            pltpu.VMEM(pressure.shape, jnp.float32),
            pltpu.VMEM((2, cells, depth, members), jnp.float32),
        ),
        in_specs=[any_space] * 3,
        out_specs=(vmem_space, vmem_space),
        scratch_shapes=[
            pltpu.VMEM((planes + 2, cells, depth, members), jnp.float32),
            pltpu.VMEM((planes + 2, cells, depth, members), jnp.float32),
            pltpu.VMEM((STEPS, 2, planes, depth, members), jnp.float32),
            pltpu.VMEM((STEPS, 2, planes, cells, TILE, members), jnp.float32),
            pltpu.VMEM((rows, cells, tiles, 2, TILE, members), jnp.float32),
            dma((STEPS, 2, tiles)), dma((STEPS, 2, tiles)),
            dma((STEPS, 2)), dma((STEPS, 2)),
            dma((STEPS, 2)), dma((STEPS, 2)),
            dma((cells, tiles, rows - 1)), dma((cells, tiles, rows - 1)),
            dma((3,)),
        ],
        compiler_params=pltpu.CompilerParams(
            collective_id=0, has_side_effects=True, vmem_limit_bytes=46 * 1024 * 1024
        ),
    )(pressure, earlier, speed_square)

    parts = 8
    return pl.pallas_call(
        rescale,
        out_shape=(jax.ShapeDtypeStruct(pressure.shape, jnp.float32),) * 2,
        in_specs=[vmem_space, vmem_space],
        out_specs=(any_space, any_space),
        scratch_shapes=[pltpu.VMEM(pressure.shape, jnp.float32), dma((parts,)), dma((parts,))],
        compiler_params=pltpu.CompilerParams(vmem_limit_bytes=24 * 1024 * 1024),
    )(end, stat)


def solution(mesh):
    spec = P("rows", "cols", "slabs", None)
    sizes = tuple(mesh.shape[name] for name in ("rows", "cols", "slabs"))
    return jax.shard_map(functools.partial(shards, sizes), mesh=mesh,
                         in_specs=(spec,) * 3, out_specs=(spec,) * 2, check_vma=False)
```
